64 devices in a mesh: dp: 8 (over x, y, core), sp: 8 (over z).
Axes of the slice: x: 2, y: 2, z: 8, core: 2. Of those that a mesh axis runs over, the one named last changes fastest.
The devices are a block of a 4x4x8 slice.
Arguments:
- q: bfloat16 [256, 16, 128], P('dp'), parts along dimension 0
- k: bfloat16 [256, 2048, 16, 128], P('dp', 'sp'), parts along dimension 0
- v: bfloat16 [256, 2048, 16, 128], P('dp', 'sp'), parts along dimension 0
Outputs:
- q: bfloat16 [256, 16, 128], P('dp'), parts along dimension 0
There are 8 independent parts. The reference program is written for one: setup_inputs(seed, part) draws one part's arguments, and reference() takes and returns one part's arrays. A program takes and returns all parts, laid end to end along the dimension named above; each array names one.
All inputs are finite; a program needn't handle non-finite values.
Results may differ from the reference program's by a relative error of at most 0.012.
Values are sent between devices in bfloat16 or wider.
A program may use at most 768 MiB of HBM per device.

```python
import jax
import jax.numpy as jnp

BATCH = 32
CACHE = 2048
HEADS = 16
KV_HEADS = 16
HEAD = 128


def setup_inputs(seed: int = 0, part: int = 0) -> dict:
    kq, kk, kv = (jax.random.fold_in(k, part) for k in jax.random.split(jax.random.key(seed), 3))
    return {
        "q": (3 * jax.random.normal(kq, (BATCH, HEADS, HEAD), jnp.float32)).astype(jnp.bfloat16),
        "k": jax.random.normal(kk, (BATCH, CACHE, KV_HEADS, HEAD), jnp.float32).astype(jnp.bfloat16),
        "v": jax.random.normal(kv, (BATCH, CACHE, KV_HEADS, HEAD), jnp.float32).astype(jnp.bfloat16),
    }


def einsum(form, a, b):
    return jnp.einsum(form, a.astype(jnp.float32), b.astype(jnp.float32))


def reference(q, k, v):
    grouped = q.reshape(BATCH, KV_HEADS, -1, HEAD)
    scores = einsum("bgsd,bugd->bgsu", grouped, k) * HEAD**-0.5
    weights = jax.nn.softmax(scores, -1).astype(jnp.bfloat16)
    return einsum("bgsu,bugd->bgsd", weights, v).astype(jnp.bfloat16).reshape(BATCH, HEADS, HEAD)
```

```python
import functools

import jax
import jax.numpy as jnp
from jax import lax
from jax.experimental import pallas as pl
from jax.experimental.pallas import tpu as pltpu
from jax.sharding import PartitionSpec as P

LOG2E = 1.4426950408889634
SLOTS = 12
LANES = 128
MESH = pl.DeviceIdType.MESH


def kernel(axis, devices, rounds, q_hbm, k_hbm, v_hbm, o_ref, *scratch):
    (qbuf, kbuf, vbuf, sbuf, hbuf, pbuf, part, stat, rpart, rstat, tpart, tstat, cols, obuf,
     qsem, ksem, vsem, psend, precv, ssend, srecv, tpsend, tprecv, tssend, tsrecv, gsend, grecv) = scratch
    n, heads, head = q_hbm.shape
    half = k_hbm.shape[2]
    chunks = half // LANES
    shared = rounds * devices
    me = lax.axis_index(axis)
    others = sorted(range(1, devices), key=lambda d: -min(d, devices - d))
    factor = head ** -0.5 * LOG2E

    def peer(d):
        return lax.rem(me + d, devices)

    def to(src, dst, send, recv, device):
        return pltpu.make_async_remote_copy(src, dst, send, recv, device_id={axis: device}, device_id_type=MESH)

    def await_bytes(ref, sem):
        pltpu.make_async_copy(ref, ref, sem).wait()

    def kcopy(i):
        return pltpu.make_async_copy(k_hbm.at[i], kbuf.at[lax.rem(i, SLOTS)], ksem.at[lax.rem(i, SLOTS)])

    def vcopy(i):
        return pltpu.make_async_copy(v_hbm.at[i], vbuf.at[lax.rem(i, SLOTS)], vsem.at[lax.rem(i, SLOTS)])

    row = lax.broadcasted_iota(jnp.int32, (2 * heads, LANES), 0)
    lane = lax.broadcasted_iota(jnp.int32, (2 * heads, LANES), 1)
    keep = lax.rem(row, heads) == lax.rem(lane, heads)
    own = keep[:heads]
    first = row[:heads] == lane[:heads]

    def scores(i):
        q = qbuf[i]
        z = jnp.zeros_like(q)
        qq = jnp.concatenate([jnp.concatenate([q, z], 1), jnp.concatenate([z, q], 1)], 0)
        slot = lax.rem(i, SLOTS)
        kk = jnp.concatenate([kbuf[slot, 0], kbuf[slot, 1]], 1)
        s = lax.dot_general(qq, kk, (((1,), (1,)), ((), ())), preferred_element_type=jnp.float32)
        cs = [jnp.where(keep, s[:, c * LANES:(c + 1) * LANES], -jnp.inf) for c in range(chunks)]
        high = functools.reduce(jnp.maximum, cs)
        return cs, jnp.maximum(high[:heads], high[heads:])

    def put_scores(cs, high):
        for c in range(chunks):
            sbuf[:, c * LANES:(c + 1) * LANES] = cs[c]
        hbuf[...] = high

    def weigh():
        high = jnp.max(hbuf[...], 1, keepdims=True) * factor
        both = jnp.broadcast_to(jnp.concatenate([high, high], 0), (2 * heads, LANES))
        ps = [jnp.exp2(sbuf[:, c * LANES:(c + 1) * LANES] * factor - both) for c in range(chunks)]
        total = functools.reduce(jnp.add, ps)
        total = jnp.sum(total[:heads] + total[heads:], 1, keepdims=True)
        as_row = lambda x: jnp.sum(jnp.where(own, jnp.broadcast_to(x, (heads, LANES)), 0.0), 0, keepdims=True)
        return [p.astype(jnp.bfloat16) for p in ps], jnp.concatenate([as_row(high), as_row(total)], 0)

    def put_weights(ps):
        for c in range(chunks):
            pbuf[:, c * LANES:(c + 1) * LANES] = ps[c]

    def seen(i):
        slot = lax.rem(i, SLOTS)
        vv = jnp.concatenate([vbuf[slot, 0], vbuf[slot, 1]], 1)
        o = jnp.dot(pbuf[...], vv, preferred_element_type=jnp.float32)
        return (o[:heads, :head] + o[heads:, head:]).astype(jnp.bfloat16)

    def step(i, put_stat, put_part):
        kcopy(i + 2).wait()
        vcopy(i).wait()
        cs, high = scores(i + 2)
        ps, st = weigh()
        put_part(i, seen(i))
        put_stat(i + 1, st)
        put_scores(cs, high)
        put_weights(ps)

        @pl.when(i + 2 + SLOTS < n)
        def _():
            kcopy(i + 2 + SLOTS).start()

        @pl.when(i + SLOTS < n)
        def _():
            vcopy(i + SLOTS).start()

    def put_stat(i, st):
        stat[i] = st

    def put_part(i, x):
        part[i] = x

    def put_tail_stat(i, st):
        tstat[i - shared, me] = st

    def put_tail_part(i, x):
        tpart[i - shared, me] = x

    def send_round(g):
        for d in others:
            p = peer(d)
            to(stat.at[g * devices + p], rstat.at[g, me], ssend.at[g], srecv.at[g], p).start()
            to(part.at[g * devices + p], rpart.at[g, me], psend.at[g], precv.at[g], p).start()
        rstat[g, me] = stat[g * devices + me]
        rpart[g, me] = part[g * devices + me]

    def shares(st):
        high, total = st[:, 0, :], st[:, 1, :]
        e = jnp.exp2(high - jnp.max(high, 0, keepdims=True))
        w = e / jnp.sum(e * total, 0, keepdims=True)
        return [jnp.sum(jnp.where(first, jnp.broadcast_to(w[d:d + 1], (heads, LANES)), 0.0), 1, keepdims=True) for d in range(devices)]

    def join_round(g):
        await_bytes(rstat.at[g, pl.ds(0, devices - 1)], srecv.at[g])
        await_bytes(rpart.at[g, pl.ds(0, devices - 1)], precv.at[g])
        w = shares(rstat[g])
        i = g * devices + me
        obuf[i] = functools.reduce(jnp.add, [rpart[g, d].astype(jnp.float32) * w[d] for d in range(devices)]).astype(jnp.bfloat16)
        for d in others:
            to(obuf.at[i], obuf.at[i], gsend.at[g], grecv.at[g], peer(d)).start()

    def send_tail_stat(i):
        t = i - shared
        for d in others:
            to(tstat.at[t, me], tstat.at[t, me], tssend.at[t], tsrecv.at[t], peer(d)).start()

    def send_tail_part(i):
        t = i - shared
        for d in others:
            to(tpart.at[t, me], tpart.at[t, me], tpsend.at[t], tprecv.at[t], peer(d)).start()

    qcopy = pltpu.make_async_copy(q_hbm, qbuf, qsem)
    qcopy.start()
    kcopy(0).start()
    kcopy(1).start()

    @pl.loop(0, SLOTS - 2)
    def _(i):
        kcopy(i + 2).start()
        vcopy(i).start()

    vcopy(SLOTS - 2).start()
    vcopy(SLOTS - 1).start()
    barrier = pltpu.get_barrier_semaphore()
    for d in others:
        pl.semaphore_signal(barrier, inc=1, device_id={axis: peer(d)}, device_id_type=MESH)
    qcopy.wait()
    kcopy(0).wait()
    put_scores(*scores(0))
    kcopy(1).wait()
    cs, high = scores(1)
    ps, st = weigh()
    put_stat(0, st)
    put_scores(cs, high)
    put_weights(ps)
    kcopy(SLOTS).start()
    kcopy(SLOTS + 1).start()

    for g in range(rounds):
        last = g == rounds - 1

        @pl.loop(g * devices, (g + 1) * devices - last)
        def _(i):
            step(i, put_stat, put_part)

        if last:
            step(shared - 1, put_tail_stat, put_part)
        if g == 0:
            pl.semaphore_wait(barrier, devices - 1)
        send_round(g)
        if g:
            join_round(g - 1)

    send_tail_stat(shared)

    @pl.loop(shared, n - 2)
    def _(i):
        step(i, put_tail_stat, put_tail_part)
        send_tail_stat(i + 1)
        send_tail_part(i)

    vcopy(n - 2).wait()
    ps, st = weigh()
    put_tail_stat(n - 1, st)
    put_tail_part(n - 2, seen(n - 2))
    put_weights(ps)
    send_tail_stat(n - 1)
    send_tail_part(n - 2)
    join_round(rounds - 1)
    vcopy(n - 1).wait()
    put_tail_part(n - 1, seen(n - 1))
    send_tail_part(n - 1)

    @pl.loop(0, n - shared)
    def _(t):
        await_bytes(tstat.at[t, pl.ds(0, devices - 1)], tsrecv.at[t])
        w = shares(tstat[t])
        for d in range(devices):
            cols[t, d] = jnp.broadcast_to(w[d], (heads, head))

    @pl.loop(0, n - shared)
    def _(t):
        await_bytes(tpart.at[t, pl.ds(0, devices - 1)], tprecv.at[t])
        o_ref[shared + t] = functools.reduce(
            jnp.add, [tpart[t, d].astype(jnp.float32) * cols[t, d] for d in range(devices)]
        ).astype(jnp.bfloat16)

    for g in range(rounds):
        await_bytes(obuf.at[pl.ds(0, devices - 1)], grecv.at[g])
        await_bytes(obuf.at[pl.ds(0, devices - 1)], gsend.at[g])
        await_bytes(rstat.at[g, pl.ds(0, devices - 1)], ssend.at[g])
        await_bytes(rpart.at[g, pl.ds(0, devices - 1)], psend.at[g])
    for i in range(shared):
        o_ref[i] = obuf[i]

    @pl.loop(0, n - shared)
    def _(t):
        await_bytes(tstat.at[t, pl.ds(0, devices - 1)], tssend.at[t])
        await_bytes(tpart.at[t, pl.ds(0, devices - 1)], tpsend.at[t])


def attend(axis, devices, q, k, v):
    n, tokens, heads, head = k.shape
    half = tokens * heads // 2
    k = k.reshape(n, 2, half, head)
    v = v.reshape(n, 2, half, head)
    rounds = n // devices - 1
    shared = rounds * devices
    tail = n - shared
    dma = pltpu.SemaphoreType.DMA
    bf16, f32 = jnp.bfloat16, jnp.float32
    return pl.pallas_call(
        functools.partial(kernel, axis, devices, rounds),
        out_shape=jax.ShapeDtypeStruct((n, heads, head), bf16),
        in_specs=[pl.BlockSpec(memory_space=pl.ANY)] * 3,
        out_specs=pl.BlockSpec(memory_space=pltpu.VMEM),
        scratch_shapes=[
            pltpu.VMEM((n, heads, head), bf16),
            pltpu.VMEM((SLOTS, 2, half, head), bf16),
            pltpu.VMEM((SLOTS, 2, half, head), bf16),
            pltpu.VMEM((2 * heads, half), f32),
            pltpu.VMEM((heads, LANES), f32),
            pltpu.VMEM((2 * heads, half), bf16),
            pltpu.VMEM((shared, heads, head), bf16),
            pltpu.VMEM((shared, 2, LANES), f32),
            pltpu.VMEM((rounds, devices, heads, head), bf16),
            pltpu.VMEM((rounds, devices, 2, LANES), f32),
            pltpu.VMEM((tail, devices, heads, head), bf16),
            pltpu.VMEM((tail, devices, 2, LANES), f32),
            pltpu.VMEM((tail, devices, heads, head), f32),
            pltpu.VMEM((shared, heads, head), bf16),
            dma, dma((SLOTS,)), dma((SLOTS,)),
            dma((rounds,)), dma((rounds,)), dma((rounds,)), dma((rounds,)),
            dma((tail,)), dma((tail,)), dma((tail,)), dma((tail,)),
            dma((rounds,)), dma((rounds,)),
        ],
        compiler_params=pltpu.CompilerParams(collective_id=0, has_side_effects=True, vmem_limit_bytes=56 << 20),
        name="attend",
    )(q, k, v)


def solution(mesh):
    def step(q, k, v):
        return attend("sp", mesh.shape["sp"], q, k, v)

    return jax.shard_map(
        step,
        mesh=mesh,
        in_specs=(P("dp", None, None), P("dp", "sp", None, None), P("dp", "sp", None, None)),
        out_specs=P("dp", None, None),
        check_vma=False,
    )
```

```python
import functools

import jax
import jax.numpy as jnp
from jax import lax
from jax.experimental import pallas as pl
from jax.experimental.pallas import tpu as pltpu
from jax.sharding import PartitionSpec as P

LOG2E = 1.4426950408889634
SLOTS = 12
LANES = 128
DIRECT = 4
EARLY = 4
LAG = 9
MESH = pl.DeviceIdType.MESH


def kernel(axis, devices, shared, q_hbm, k_hbm, v_hbm, o_ref, *scratch):
    (qbuf, kbuf, vbuf, sbuf, hbuf, pbuf, part, stat, rpart, rstat, tpart, tstat, cols, obuf,
     qsem, ksem, vsem, psend, precv, ssend, srecv, tpsend, tprecv, tssend, tsrecv, gsend, grecv) = scratch
    n, heads, head = q_hbm.shape
    half = k_hbm.shape[2]
    chunks = half // LANES
    me = lax.axis_index(axis)
    others = sorted(range(1, devices), key=lambda d: -min(d, devices - d))
    factor = head ** -0.5 * LOG2E

    def peer(d):
        return lax.rem(me + d, devices)

    def to(src, dst, send, recv, device):
        return pltpu.make_async_remote_copy(src, dst, send, recv, device_id={axis: device}, device_id_type=MESH)

    def await_bytes(ref, sem):
        pltpu.make_async_copy(ref, ref, sem).wait()

    def kcopy(i):
        return pltpu.make_async_copy(k_hbm.at[i], kbuf.at[lax.rem(i, SLOTS)], ksem.at[lax.rem(i, SLOTS)])

    def vcopy(i):
        return pltpu.make_async_copy(v_hbm.at[i], vbuf.at[lax.rem(i, SLOTS)], vsem.at[lax.rem(i, SLOTS)])

    row = lax.broadcasted_iota(jnp.int32, (2 * heads, LANES), 0)
    lane = lax.broadcasted_iota(jnp.int32, (2 * heads, LANES), 1)
    keep = lax.rem(row, heads) == lax.rem(lane, heads)
    own = keep[:heads]
    first = row[:heads] == lane[:heads]

    def scores(i):
        q = qbuf[i]
        z = jnp.zeros_like(q)
        qq = jnp.concatenate([jnp.concatenate([q, z], 1), jnp.concatenate([z, q], 1)], 0)
        slot = lax.rem(i, SLOTS)
        kk = jnp.concatenate([kbuf[slot, 0], kbuf[slot, 1]], 1)
        s = lax.dot_general(qq, kk, (((1,), (1,)), ((), ())), preferred_element_type=jnp.float32)
        cs = [jnp.where(keep, s[:, c * LANES:(c + 1) * LANES], -jnp.inf) for c in range(chunks)]
        high = functools.reduce(jnp.maximum, cs)
        return cs, jnp.maximum(high[:heads], high[heads:])

    def put_scores(t, cs, high):
        for c in range(chunks):
            sbuf[t, :, c * LANES:(c + 1) * LANES] = cs[c]
        hbuf[t] = high

    def weigh(t):
        high = jnp.max(hbuf[t], 1, keepdims=True) * factor
        both = jnp.broadcast_to(jnp.concatenate([high, high], 0), (2 * heads, LANES))
        ps = [jnp.exp2(sbuf[t, :, c * LANES:(c + 1) * LANES] * factor - both) for c in range(chunks)]
        total = functools.reduce(jnp.add, ps)
        total = jnp.sum(total[:heads] + total[heads:], 1, keepdims=True)
        as_row = lambda x: jnp.sum(jnp.where(own, jnp.broadcast_to(x, (heads, LANES)), 0.0), 0, keepdims=True)
        return [p.astype(jnp.bfloat16) for p in ps], jnp.concatenate([as_row(high), as_row(total)], 0)

    def put_weights(t, ps):
        for c in range(chunks):
            pbuf[t, :, c * LANES:(c + 1) * LANES] = ps[c]

    def seen(t, i):
        slot = lax.rem(i, SLOTS)
        vv = jnp.concatenate([vbuf[slot, 0], vbuf[slot, 1]], 1)
        o = sum(jnp.dot(pbuf[t, :, x:x + half // 2], vv[x:x + half // 2], preferred_element_type=jnp.float32) for x in (0, half // 2))
        return (o[:heads, :head] + o[heads:, head:]).astype(jnp.bfloat16)

    def steps(i, put_stat, put_part, put_next):
        for u in range(2):
            kcopy(i + 2 + u).wait()
            vcopy(i + u).wait()
        for u in range(2):
            cs, high = scores(i + 2 + u)
            ps, st = weigh(1 - u)
            put_part(i + u, seen(u, i + u))
            (put_next if u else put_stat)(i + 1 + u, st)
            put_scores(u, cs, high)
            put_weights(1 - u, ps)

        for u in range(2):
            @pl.when(i + u + 2 + SLOTS < n)
            def _():
                kcopy(i + u + 2 + SLOTS).start()

            @pl.when(i + u + SLOTS < n)
            def _():
                vcopy(i + u + SLOTS).start()

    def put_stat(i, st):
        stat[i] = st

    def put_part(i, x):
        part[i] = x

    def put_tail_stat(i, st):
        tstat[i - shared, me] = st

    def put_tail_part(i, x):
        tpart[i - shared, me] = x

    def send_owner(i):
        owner, g = lax.rem(i, devices), lax.div(i, devices)

        @pl.when(owner != me)
        def _():
            to(stat.at[i], rstat.at[g, me], ssend.at[i], srecv.at[g], owner).start()
            to(part.at[i], rpart.at[g, me], psend.at[i], precv.at[g], owner).start()

    def shares(st):
        high, total = st[:, 0, :], st[:, 1, :]
        e = jnp.exp2(high - jnp.max(high, 0, keepdims=True))
        w = e / jnp.sum(e * total, 0, keepdims=True)
        return [jnp.sum(jnp.where(first, jnp.broadcast_to(w[d:d + 1], (heads, LANES)), 0.0), 1, keepdims=True) for d in range(devices)]

    def join(i):
        g = lax.div(i, devices)
        rstat[g, me] = stat[i]
        rpart[g, me] = part[i]
        await_bytes(rstat.at[g, pl.ds(0, devices - 1)], srecv.at[g])
        await_bytes(rpart.at[g, pl.ds(0, devices - 1)], precv.at[g])
        w = shares(rstat[g])
        obuf[i] = functools.reduce(jnp.add, [rpart[g, d].astype(jnp.float32) * w[d] for d in range(devices)]).astype(jnp.bfloat16)
        for d in others:
            to(obuf.at[i], obuf.at[i], gsend.at[g], grecv.at[i], peer(d)).start()

    def send_tail_stat(i):
        t = i - shared
        for d in others:
            to(tstat.at[t, me], tstat.at[t, me], tssend.at[t], tsrecv.at[t], peer(d)).start()

    def send_tail_part(i):
        t = i - shared
        for d in others:
            to(tpart.at[t, me], tpart.at[t, me], tpsend.at[t], tprecv.at[t], peer(d)).start()

    qcopy = pltpu.make_async_copy(q_hbm, qbuf, qsem)
    qcopy.start()
    kcopy(0).start()
    kcopy(1).start()

    @pl.loop(0, SLOTS - 2)
    def _(i):
        kcopy(i + 2).start()
        vcopy(i).start()

    vcopy(SLOTS - 2).start()
    vcopy(SLOTS - 1).start()
    barrier = pltpu.get_barrier_semaphore()
    for d in others:
        pl.semaphore_signal(barrier, inc=1, device_id={axis: peer(d)}, device_id_type=MESH)
    qcopy.wait()
    kcopy(0).wait()
    put_scores(0, *scores(0))
    kcopy(1).wait()
    cs, high = scores(1)
    ps, st = weigh(0)
    put_stat(0, st)
    put_scores(1, cs, high)
    put_weights(0, ps)
    kcopy(SLOTS).start()
    kcopy(SLOTS + 1).start()

    @pl.loop(0, EARLY, step=2)
    def _(i):
        steps(i, put_stat, put_part, put_stat)

    pl.semaphore_wait(barrier, devices - 1)

    @pl.loop(0, EARLY)
    def _(i):
        send_owner(i)

    def joint(i):
        send_owner(i)

        @pl.when(jnp.logical_and(i >= LAG, lax.rem(i - LAG + devices, devices) == me))
        def _():
            join(i - LAG)

    @pl.loop(EARLY, shared - 2, step=2)
    def _(i):
        steps(i, put_stat, put_part, put_stat)
        joint(i)
        joint(i + 1)

    steps(shared - 2, put_stat, put_part, put_tail_stat)
    joint(shared - 2)
    joint(shared - 1)
    send_tail_stat(shared)

    def late_join(i):
        @pl.when(jnp.logical_and(lax.rem(i - LAG, devices) == me, i - LAG < shared))
        def _():
            join(i - LAG)

    @pl.loop(shared, n - 2, step=2)
    def _(i):
        steps(i, put_tail_stat, put_tail_part, put_tail_stat)
        for u in range(2):
            send_tail_part(i + u)
            send_tail_stat(i + 1 + u)
        late_join(i)
        late_join(i + 1)

    vcopy(n - 2).wait()
    ps, st = weigh(1)
    put_tail_stat(n - 1, st)
    put_tail_part(n - 2, seen(0, n - 2))
    put_weights(1, ps)
    send_tail_stat(n - 1)
    send_tail_part(n - 2)
    vcopy(n - 1).wait()
    put_tail_part(n - 1, seen(1, n - 1))
    send_tail_part(n - 1)
    late_join(n - 2)

    @pl.loop(n - 1, shared + LAG)
    def _(i):
        late_join(i)

    @pl.loop(0, n - shared)
    def _(t):
        await_bytes(tstat.at[t, pl.ds(0, devices - 1)], tsrecv.at[t])
        w = shares(tstat[t])
        for d in range(devices):
            cols[t, d] = jnp.broadcast_to(w[d], (heads, head))

    @pl.loop(0, n - shared)
    def _(t):
        await_bytes(tpart.at[t, pl.ds(0, devices - 1)], tprecv.at[t])
        o_ref[shared + t] = functools.reduce(
            jnp.add, [tpart[t, d].astype(jnp.float32) * cols[t, d] for d in range(devices)]
        ).astype(jnp.bfloat16)

    @pl.loop(0, shared)
    def _(i):
        mine = lax.rem(i, devices) == me

        @pl.when(jnp.logical_not(mine))
        def _():
            await_bytes(obuf.at[i], grecv.at[i])

        o_ref[i] = obuf[i]

    @pl.loop(0, shared)
    def _(i):
        mine = lax.rem(i, devices) == me

        @pl.when(mine)
        def _():
            await_bytes(obuf.at[pl.ds(0, devices - 1)], gsend.at[lax.div(i, devices)])

        @pl.when(jnp.logical_not(mine))
        def _():
            await_bytes(stat.at[i], ssend.at[i])
            await_bytes(part.at[i], psend.at[i])

    @pl.loop(0, n - shared)
    def _(t):
        await_bytes(tstat.at[t, pl.ds(0, devices - 1)], tssend.at[t])
        await_bytes(tpart.at[t, pl.ds(0, devices - 1)], tpsend.at[t])


def attend(axis, devices, q, k, v):
    n, tokens, heads, head = k.shape
    half = tokens * heads // 2
    k = k.reshape(n, 2, half, head)
    v = v.reshape(n, 2, half, head)
    tail = DIRECT
    shared = n - tail
    rounds = -(-shared // devices)
    dma = pltpu.SemaphoreType.DMA
    bf16, f32 = jnp.bfloat16, jnp.float32
    return pl.pallas_call(
        functools.partial(kernel, axis, devices, shared),
        out_shape=pltpu.VMEM((n, heads, head), bf16),
        in_specs=[pl.BlockSpec(memory_space=pl.ANY)] * 3,
        out_specs=pl.BlockSpec(memory_space=pltpu.VMEM),
        scratch_shapes=[
            pltpu.VMEM((n, heads, head), bf16),
            pltpu.VMEM((SLOTS, 2, half, head), bf16),
            pltpu.VMEM((SLOTS, 2, half, head), bf16),
            pltpu.VMEM((2, 2 * heads, half), f32),
            pltpu.VMEM((2, heads, LANES), f32),
            pltpu.VMEM((2, 2 * heads, half), bf16),
            pltpu.VMEM((shared, heads, head), bf16),
            pltpu.VMEM((shared, 2, LANES), f32),
            pltpu.VMEM((rounds, devices, heads, head), bf16),
            pltpu.VMEM((rounds, devices, 2, LANES), f32),
            pltpu.VMEM((tail, devices, heads, head), bf16),
            pltpu.VMEM((tail, devices, 2, LANES), f32),
            pltpu.VMEM((tail, devices, heads, head), f32),
            pltpu.VMEM((shared, heads, head), bf16),
            dma, dma((SLOTS,)), dma((SLOTS,)),
            dma((shared,)), dma((rounds,)), dma((shared,)), dma((rounds,)),
            dma((tail,)), dma((tail,)), dma((tail,)), dma((tail,)),
            dma((rounds,)), dma((shared,)),
        ],
        compiler_params=pltpu.CompilerParams(collective_id=0, has_side_effects=True, vmem_limit_bytes=56 << 20),
        name="attend",
    )(q, k, v)


def solution(mesh):
    def step(q, k, v):
        return attend("sp", mesh.shape["sp"], q, k, v)

    return jax.shard_map(
        step,
        mesh=mesh,
        in_specs=(P("dp", None, None), P("dp", "sp", None, None), P("dp", "sp", None, None)),
        out_specs=P("dp", None, None),
        check_vma=False,
    )
```

```python
import functools

import jax
import jax.numpy as jnp
from jax import lax
from jax.experimental import pallas as pl
from jax.experimental.pallas import tpu as pltpu
from jax.sharding import PartitionSpec as P

LOG2E = 1.4426950408889634
SLOTS = 12
LANES = 128
DIRECT = 2
EARLY = 4
OWNERS = (2, 1, 5, 0, 6, 7, 3, 4)
LAG = 14
MESH = pl.DeviceIdType.MESH


def kernel(axis, devices, shared, q_hbm, k_hbm, v_hbm, o_ref, *scratch):
    (qbuf, kbuf, vbuf, sbuf, hbuf, pbuf, part, stat, rpart, rstat, tpart, tstat, cols,
     qsem, ksem, vsem, psend, precv, ssend, srecv, tpsend, tprecv, tssend, tsrecv, gsend, grecv) = scratch
    n, heads, head = q_hbm.shape
    half = k_hbm.shape[2]
    chunks = half // LANES
    me = lax.axis_index(axis)
    others = sorted(range(1, devices), key=lambda d: -min(d, devices - d))
    factor = head ** -0.5 * LOG2E

    pick = lambda table, x: sum(jnp.where(x == j, y, 0) for j, y in enumerate(table))
    place = pick([OWNERS.index(d) for d in range(devices)], me)

    def peer(d):
        return lax.rem(me + d, devices)

    def to(src, dst, send, recv, device):
        return pltpu.make_async_remote_copy(src, dst, send, recv, device_id={axis: device}, device_id_type=MESH)

    def await_bytes(ref, sem):
        pltpu.make_async_copy(ref, ref, sem).wait()

    def kcopy(i):
        return pltpu.make_async_copy(k_hbm.at[i], kbuf.at[lax.rem(i, SLOTS)], ksem.at[lax.rem(i, SLOTS)])

    def vcopy(i):
        return pltpu.make_async_copy(v_hbm.at[i], vbuf.at[lax.rem(i, SLOTS)], vsem.at[lax.rem(i, SLOTS)])

    row = lax.broadcasted_iota(jnp.int32, (2 * heads, LANES), 0)
    lane = lax.broadcasted_iota(jnp.int32, (2 * heads, LANES), 1)
    keep = lax.rem(row, heads) == lax.rem(lane, heads)
    own = keep[:heads]
    first = row[:heads] == lane[:heads]

    def scores(i):
        q = qbuf[i]
        z = jnp.zeros_like(q)
        qq = jnp.concatenate([jnp.concatenate([q, z], 1), jnp.concatenate([z, q], 1)], 0)
        slot = lax.rem(i, SLOTS)
        kk = jnp.concatenate([kbuf[slot, 0], kbuf[slot, 1]], 1)
        s = lax.dot_general(qq, kk, (((1,), (1,)), ((), ())), preferred_element_type=jnp.float32)
        cs = [jnp.where(keep, s[:, c * LANES:(c + 1) * LANES], -jnp.inf) for c in range(chunks)]
        high = functools.reduce(jnp.maximum, cs)
        return cs, jnp.maximum(high[:heads], high[heads:])

    def put_scores(t, cs, high):
        for c in range(chunks):
            sbuf[t, :, c * LANES:(c + 1) * LANES] = cs[c]
        hbuf[t] = high

    def weigh(t):
        high = jnp.max(hbuf[t], 1, keepdims=True) * factor
        both = jnp.broadcast_to(jnp.concatenate([high, high], 0), (2 * heads, LANES))
        ps = [jnp.exp2(sbuf[t, :, c * LANES:(c + 1) * LANES] * factor - both) for c in range(chunks)]
        total = functools.reduce(jnp.add, ps)
        total = jnp.sum(total[:heads] + total[heads:], 1, keepdims=True)
        as_row = lambda x: jnp.sum(jnp.where(own, jnp.broadcast_to(x, (heads, LANES)), 0.0), 0, keepdims=True)
        return [p.astype(jnp.bfloat16) for p in ps], jnp.concatenate([as_row(high), as_row(total)], 0)

    def put_weights(t, ps):
        for c in range(chunks):
            pbuf[t, :, c * LANES:(c + 1) * LANES] = ps[c]

    def seen(t, i):
        slot = lax.rem(i, SLOTS)
        vv = jnp.concatenate([vbuf[slot, 0], vbuf[slot, 1]], 1)
        o = sum(jnp.dot(pbuf[t, :, x:x + half // 2], vv[x:x + half // 2], preferred_element_type=jnp.float32) for x in (0, half // 2))
        return (o[:heads, :head] + o[heads:, head:]).astype(jnp.bfloat16)

    def steps(i, put_stat, put_part, put_next):
        for u in range(2):
            kcopy(i + 2 + u).wait()
            vcopy(i + u).wait()
        for u in range(2):
            cs, high = scores(i + 2 + u)
            ps, st = weigh(1 - u)
            put_part(i + u, seen(u, i + u))
            (put_next if u else put_stat)(i + 1 + u, st)
            put_scores(u, cs, high)
            put_weights(1 - u, ps)

        for u in range(2):
            @pl.when(i + u + 2 + SLOTS < n)
            def _():
                kcopy(i + u + 2 + SLOTS).start()

            @pl.when(i + u + SLOTS < n)
            def _():
                vcopy(i + u + SLOTS).start()

    def put_stat(i, st):
        stat[i] = st

    def put_part(i, x):
        part[i] = x

    def put_tail_stat(i, st):
        tstat[i - shared, me] = st

    def put_tail_part(i, x):
        tpart[i - shared, me] = x

    def send_owner(i):
        owner, g = pick(OWNERS, lax.rem(i, devices)), lax.div(i, devices)

        @pl.when(owner != me)
        def _():
            to(stat.at[i], rstat.at[g, me], ssend.at[i], srecv.at[g], owner).start()
            to(part.at[i], rpart.at[g, me], psend.at[i], precv.at[g], owner).start()

    def shares(st):
        high, total = st[:, 0, :], st[:, 1, :]
        e = jnp.exp2(high - jnp.max(high, 0, keepdims=True))
        w = e / jnp.sum(e * total, 0, keepdims=True)
        return [jnp.sum(jnp.where(first, jnp.broadcast_to(w[d:d + 1], (heads, LANES)), 0.0), 1, keepdims=True) for d in range(devices)]

    def join(i):
        g = lax.div(i, devices)
        rstat[g, me] = stat[i]
        rpart[g, me] = part[i]
        await_bytes(rstat.at[g, pl.ds(0, devices - 1)], srecv.at[g])
        await_bytes(rpart.at[g, pl.ds(0, devices - 1)], precv.at[g])
        w = shares(rstat[g])
        o_ref[i] = functools.reduce(jnp.add, [rpart[g, d].astype(jnp.float32) * w[d] for d in range(devices)]).astype(jnp.bfloat16)
        for d in others:
            to(o_ref.at[i], o_ref.at[i], gsend.at[g], grecv.at[i], peer(d)).start()

    def send_tail_stat(i):
        t = i - shared
        for d in others:
            to(tstat.at[t, me], tstat.at[t, me], tssend.at[t], tsrecv.at[t], peer(d)).start()

    def send_tail_part(i):
        t = i - shared
        for d in others:
            to(tpart.at[t, me], tpart.at[t, me], tpsend.at[t], tprecv.at[t], peer(d)).start()

    qcopy = pltpu.make_async_copy(q_hbm, qbuf, qsem)
    qcopy.start()
    kcopy(0).start()
    kcopy(1).start()

    @pl.loop(0, SLOTS - 2)
    def _(i):
        kcopy(i + 2).start()
        vcopy(i).start()

    vcopy(SLOTS - 2).start()
    vcopy(SLOTS - 1).start()
    barrier = pltpu.get_barrier_semaphore()
    for d in others:
        pl.semaphore_signal(barrier, inc=1, device_id={axis: peer(d)}, device_id_type=MESH)
    qcopy.wait()
    kcopy(0).wait()
    put_scores(0, *scores(0))
    kcopy(1).wait()
    cs, high = scores(1)
    ps, st = weigh(0)
    put_stat(0, st)
    put_scores(1, cs, high)
    put_weights(0, ps)
    kcopy(SLOTS).start()
    kcopy(SLOTS + 1).start()

    @pl.loop(0, EARLY, step=2)
    def _(i):
        steps(i, put_stat, put_part, put_stat)

    pl.semaphore_wait(barrier, devices - 1)

    @pl.loop(0, EARLY)
    def _(i):
        send_owner(i)

    def joint(i):
        send_owner(i)

        @pl.when(jnp.logical_and(i >= LAG, lax.rem(i - LAG + devices, devices) == place))
        def _():
            join(i - LAG)

    @pl.loop(EARLY, shared - 2, step=2)
    def _(i):
        steps(i, put_stat, put_part, put_stat)
        joint(i)
        joint(i + 1)

    steps(shared - 2, put_stat, put_part, put_tail_stat)
    joint(shared - 2)
    joint(shared - 1)
    send_tail_stat(shared)

    def late_join(i):
        @pl.when(jnp.logical_and(lax.rem(i - LAG, devices) == place, i - LAG < shared))
        def _():
            join(i - LAG)

    @pl.loop(shared, n - 2, step=2)
    def _(i):
        steps(i, put_tail_stat, put_tail_part, put_tail_stat)
        for u in range(2):
            send_tail_part(i + u)
            send_tail_stat(i + 1 + u)
        late_join(i)
        late_join(i + 1)

    vcopy(n - 2).wait()
    ps, st = weigh(1)
    put_tail_stat(n - 1, st)
    put_tail_part(n - 2, seen(0, n - 2))
    put_weights(1, ps)
    send_tail_stat(n - 1)
    send_tail_part(n - 2)
    vcopy(n - 1).wait()
    put_tail_part(n - 1, seen(1, n - 1))
    send_tail_part(n - 1)
    late_join(n - 2)

    @pl.loop(n - 1, shared + LAG)
    def _(i):
        late_join(i)

    @pl.loop(0, n - shared)
    def _(t):
        await_bytes(tstat.at[t, pl.ds(0, devices - 1)], tsrecv.at[t])
        w = shares(tstat[t])
        for d in range(devices):
            cols[t, d] = jnp.broadcast_to(w[d], (heads, head))

    def settle(i):
        @pl.when(lax.rem(i, devices) == place)
        def _():
            await_bytes(o_ref.at[pl.ds(0, devices - 1)], gsend.at[lax.div(i, devices)])

        @pl.when(lax.rem(i, devices) != place)
        def _():
            await_bytes(stat.at[i], ssend.at[i])
            await_bytes(part.at[i], psend.at[i])
            await_bytes(o_ref.at[i], grecv.at[i])

    @pl.loop(0, shared - devices)
    def _(i):
        settle(i)

    @pl.loop(0, n - shared)
    def _(t):
        await_bytes(tpart.at[t, pl.ds(0, devices - 1)], tprecv.at[t])
        o_ref[shared + t] = functools.reduce(
            jnp.add, [tpart[t, d].astype(jnp.float32) * cols[t, d] for d in range(devices)]
        ).astype(jnp.bfloat16)
        await_bytes(tstat.at[t, pl.ds(0, devices - 1)], tssend.at[t])
        await_bytes(tpart.at[t, pl.ds(0, devices - 1)], tpsend.at[t])

    @pl.loop(shared - devices, shared)
    def _(i):
        settle(i)


def attend(axis, devices, q, k, v):
    n, tokens, heads, head = k.shape
    half = tokens * heads // 2
    k = k.reshape(n, 2, half, head)
    v = v.reshape(n, 2, half, head)
    tail = DIRECT
    shared = n - tail
    rounds = -(-shared // devices)
    dma = pltpu.SemaphoreType.DMA
    bf16, f32 = jnp.bfloat16, jnp.float32
    return pl.pallas_call(
        functools.partial(kernel, axis, devices, shared),
        out_shape=pltpu.VMEM((n, heads, head), bf16),
        in_specs=[pl.BlockSpec(memory_space=pl.ANY)] * 3,
        out_specs=pl.BlockSpec(memory_space=pltpu.VMEM),
        scratch_shapes=[
            pltpu.VMEM((n, heads, head), bf16),
            pltpu.VMEM((SLOTS, 2, half, head), bf16),
            pltpu.VMEM((SLOTS, 2, half, head), bf16),
            pltpu.VMEM((2, 2 * heads, half), f32),
            pltpu.VMEM((2, heads, LANES), f32),
            pltpu.VMEM((2, 2 * heads, half), bf16),
            pltpu.VMEM((shared, heads, head), bf16),
            pltpu.VMEM((shared, 2, LANES), f32),
            pltpu.VMEM((rounds, devices, heads, head), bf16),
            pltpu.VMEM((rounds, devices, 2, LANES), f32),
            pltpu.VMEM((tail, devices, heads, head), bf16),
            pltpu.VMEM((tail, devices, 2, LANES), f32),
            pltpu.VMEM((tail, devices, heads, head), f32),
            dma, dma((SLOTS,)), dma((SLOTS,)),
            dma((shared,)), dma((rounds,)), dma((shared,)), dma((rounds,)),
            dma((tail,)), dma((tail,)), dma((tail,)), dma((tail,)),
            dma((rounds,)), dma((shared,)),
        ],
        compiler_params=pltpu.CompilerParams(collective_id=0, has_side_effects=True, vmem_limit_bytes=56 << 20),
        name="attend",
    )(q, k, v)


def solution(mesh):
    def step(q, k, v):
        return attend("sp", mesh.shape["sp"], q, k, v)

    return jax.shard_map(
        step,
        mesh=mesh,
        in_specs=(P("dp", None, None), P("dp", "sp", None, None), P("dp", "sp", None, None)),
        out_specs=P("dp", None, None),
        check_vma=False,
    )
```

```python
import functools

import jax
import jax.numpy as jnp
from jax import lax
from jax.experimental import pallas as pl
from jax.experimental.pallas import tpu as pltpu
from jax.sharding import PartitionSpec as P

LOG2E = 1.4426950408889634
SLOTS = 12
LANES = 128
DIRECT = 2
EARLY = 4
OWNERS = (2, 1, 5, 0, 6, 7, 3, 4)
LAG = 14
MESH = pl.DeviceIdType.MESH


def kernel(axis, devices, shared, q_hbm, k_hbm, v_hbm, o_ref, *scratch):
    (qbuf, kbuf, vbuf, sbuf, hbuf, pbuf, part, stat, rpart, rstat, tpart, tstat, cols,
     qsem, ksem, vsem, psend, precv, ssend, srecv, tpsend, tprecv, tssend, tsrecv, gsend, grecv) = scratch
    n, heads, head = q_hbm.shape
    half = k_hbm.shape[2]
    chunks = half // LANES
    me = lax.axis_index(axis)
    others = range(devices - 1)
    factor = head ** -0.5 * LOG2E

    pick = lambda table, x: sum(jnp.where(x == j, y, 0) for j, y in enumerate(table))
    place = pick([OWNERS.index(d) for d in range(devices)], me)

    def peer(d):
        return jnp.where(d >= me, d + 1, d)

    def to(src, dst, send, recv, device):
        return pltpu.make_async_remote_copy(src, dst, send, recv, device_id={axis: device}, device_id_type=MESH)

    def await_bytes(ref, sem):
        pltpu.make_async_copy(ref, ref, sem).wait()

    def kcopy(i):
        return pltpu.make_async_copy(k_hbm.at[i], kbuf.at[lax.rem(i, SLOTS)], ksem.at[lax.rem(i, SLOTS)])

    def vcopy(i):
        return pltpu.make_async_copy(v_hbm.at[i], vbuf.at[lax.rem(i, SLOTS)], vsem.at[lax.rem(i, SLOTS)])

    row = lax.broadcasted_iota(jnp.int32, (2 * heads, LANES), 0)
    lane = lax.broadcasted_iota(jnp.int32, (2 * heads, LANES), 1)
    keep = lax.rem(row, heads) == lax.rem(lane, heads)
    own = keep[:heads]
    first = row[:heads] == lane[:heads]

    def scores(i):
        q = qbuf[i]
        z = jnp.zeros_like(q)
        qq = jnp.concatenate([jnp.concatenate([q, z], 1), jnp.concatenate([z, q], 1)], 0)
        slot = lax.rem(i, SLOTS)
        kk = jnp.concatenate([kbuf[slot, 0], kbuf[slot, 1]], 1)
        s = lax.dot_general(qq, kk, (((1,), (1,)), ((), ())), preferred_element_type=jnp.float32)
        cs = [jnp.where(keep, s[:, c * LANES:(c + 1) * LANES], -jnp.inf) for c in range(chunks)]
        high = functools.reduce(jnp.maximum, cs)
        return cs, jnp.maximum(high[:heads], high[heads:])

    def put_scores(t, cs, high):
        for c in range(chunks):
            sbuf[t, :, c * LANES:(c + 1) * LANES] = cs[c]
        hbuf[t] = high

    def weigh(t):
        high = jnp.max(hbuf[t], 1, keepdims=True) * factor
        both = jnp.broadcast_to(jnp.concatenate([high, high], 0), (2 * heads, LANES))
        ps = [jnp.exp2(sbuf[t, :, c * LANES:(c + 1) * LANES] * factor - both) for c in range(chunks)]
        total = functools.reduce(jnp.add, ps)
        total = jnp.sum(total[:heads] + total[heads:], 1, keepdims=True)
        as_row = lambda x: jnp.sum(jnp.where(own, jnp.broadcast_to(x, (heads, LANES)), 0.0), 0, keepdims=True)
        return [p.astype(jnp.bfloat16) for p in ps], jnp.concatenate([as_row(high), as_row(total)], 0)

    def put_weights(t, ps):
        for c in range(chunks):
            pbuf[t, :, c * LANES:(c + 1) * LANES] = ps[c]

    def seen(t, i):
        slot = lax.rem(i, SLOTS)
        vv = jnp.concatenate([vbuf[slot, 0], vbuf[slot, 1]], 1)
        o = sum(jnp.dot(pbuf[t, :, x:x + half // 2], vv[x:x + half // 2], preferred_element_type=jnp.float32) for x in (0, half // 2))
        return (o[:heads, :head] + o[heads:, head:]).astype(jnp.bfloat16)

    def steps(i, put_stat, put_part, put_next):
        for u in range(2):
            kcopy(i + 2 + u).wait()
            vcopy(i + u).wait()
        for u in range(2):
            cs, high = scores(i + 2 + u)
            ps, st = weigh(1 - u)
            put_part(i + u, seen(u, i + u))
            (put_next if u else put_stat)(i + 1 + u, st)
            put_scores(u, cs, high)
            put_weights(1 - u, ps)

        for u in range(2):
            @pl.when(i + u + 2 + SLOTS < n)
            def _():
                kcopy(i + u + 2 + SLOTS).start()

            @pl.when(i + u + SLOTS < n)
            def _():
                vcopy(i + u + SLOTS).start()

    def put_stat(i, st):
        stat[i] = st

    def put_part(i, x):
        part[i] = x

    def put_tail_stat(i, st):
        tstat[i - shared, me] = st

    def put_tail_part(i, x):
        tpart[i - shared, me] = x

    def send_owner(i):
        owner, g = pick(OWNERS, lax.rem(i, devices)), lax.div(i, devices)

        @pl.when(owner != me)
        def _():
            to(stat.at[i], rstat.at[g, me], ssend.at[i], srecv.at[g], owner).start()
            to(part.at[i], rpart.at[g, me], psend.at[i], precv.at[g], owner).start()

    def shares(st):
        high, total = st[:, 0, :], st[:, 1, :]
        e = jnp.exp2(high - jnp.max(high, 0, keepdims=True))
        w = e / jnp.sum(e * total, 0, keepdims=True)
        return [jnp.sum(jnp.where(first, jnp.broadcast_to(w[d:d + 1], (heads, LANES)), 0.0), 1, keepdims=True) for d in range(devices)]

    def join(i):
        g = lax.div(i, devices)
        rstat[g, me] = stat[i]
        rpart[g, me] = part[i]
        await_bytes(rstat.at[g, pl.ds(0, devices - 1)], srecv.at[g])
        await_bytes(rpart.at[g, pl.ds(0, devices - 1)], precv.at[g])
        w = shares(rstat[g])
        o_ref[i] = functools.reduce(jnp.add, [rpart[g, d].astype(jnp.float32) * w[d] for d in range(devices)]).astype(jnp.bfloat16)
        for d in others:
            to(o_ref.at[i], o_ref.at[i], gsend.at[g], grecv.at[i], peer(d)).start()

    def send_tail_stat(i):
        t = i - shared
        for d in others:
            to(tstat.at[t, me], tstat.at[t, me], tssend.at[t], tsrecv.at[t], peer(d)).start()

    def send_tail_part(i):
        t = i - shared
        for d in others:
            to(tpart.at[t, me], tpart.at[t, me], tpsend.at[t], tprecv.at[t], peer(d)).start()

    qcopy = pltpu.make_async_copy(q_hbm, qbuf, qsem)
    qcopy.start()
    kcopy(0).start()
    kcopy(1).start()

    @pl.loop(0, SLOTS - 2)
    def _(i):
        kcopy(i + 2).start()
        vcopy(i).start()

    vcopy(SLOTS - 2).start()
    vcopy(SLOTS - 1).start()
    barrier = pltpu.get_barrier_semaphore()
    for d in others:
        pl.semaphore_signal(barrier, inc=1, device_id={axis: peer(d)}, device_id_type=MESH)
    qcopy.wait()
    kcopy(0).wait()
    put_scores(0, *scores(0))
    kcopy(1).wait()
    cs, high = scores(1)
    ps, st = weigh(0)
    put_stat(0, st)
    put_scores(1, cs, high)
    put_weights(0, ps)
    kcopy(SLOTS).start()
    kcopy(SLOTS + 1).start()

    @pl.loop(0, EARLY, step=2)
    def _(i):
        steps(i, put_stat, put_part, put_stat)

    pl.semaphore_wait(barrier, devices - 1)

    @pl.loop(0, EARLY)
    def _(i):
        send_owner(i)

    def joint(i):
        send_owner(i)

        @pl.when(jnp.logical_and(i >= LAG, lax.rem(i - LAG + devices, devices) == place))
        def _():
            join(i - LAG)

    @pl.loop(EARLY, shared - 2, step=2)
    def _(i):
        steps(i, put_stat, put_part, put_stat)
        joint(i)
        joint(i + 1)

    steps(shared - 2, put_stat, put_part, put_tail_stat)
    joint(shared - 2)
    joint(shared - 1)
    send_tail_stat(shared)

    def late_join(i):
        @pl.when(jnp.logical_and(lax.rem(i - LAG, devices) == place, i - LAG < shared))
        def _():
            join(i - LAG)

    @pl.loop(shared, n - 2, step=2)
    def _(i):
        steps(i, put_tail_stat, put_tail_part, put_tail_stat)
        for u in range(2):
            send_tail_part(i + u)
            send_tail_stat(i + 1 + u)
        late_join(i)
        late_join(i + 1)

    vcopy(n - 2).wait()
    ps, st = weigh(1)
    put_tail_stat(n - 1, st)
    put_tail_part(n - 2, seen(0, n - 2))
    put_weights(1, ps)
    send_tail_stat(n - 1)
    send_tail_part(n - 2)
    vcopy(n - 1).wait()
    put_tail_part(n - 1, seen(1, n - 1))
    send_tail_part(n - 1)
    late_join(n - 2)

    @pl.loop(n - 1, shared + LAG)
    def _(i):
        late_join(i)

    @pl.loop(0, n - shared)
    def _(t):
        await_bytes(tstat.at[t, pl.ds(0, devices - 1)], tsrecv.at[t])
        w = shares(tstat[t])
        for d in range(devices):
            cols[t, d] = jnp.broadcast_to(w[d], (heads, head))

    def settle(i):
        @pl.when(lax.rem(i, devices) == place)
        def _():
            await_bytes(o_ref.at[pl.ds(0, devices - 1)], gsend.at[lax.div(i, devices)])

        @pl.when(lax.rem(i, devices) != place)
        def _():
            await_bytes(stat.at[i], ssend.at[i])
            await_bytes(part.at[i], psend.at[i])
            await_bytes(o_ref.at[i], grecv.at[i])

    @pl.loop(0, shared - devices)
    def _(i):
        settle(i)

    @pl.loop(0, n - shared)
    def _(t):
        await_bytes(tpart.at[t, pl.ds(0, devices - 1)], tprecv.at[t])
        o_ref[shared + t] = functools.reduce(
            jnp.add, [tpart[t, d].astype(jnp.float32) * cols[t, d] for d in range(devices)]
        ).astype(jnp.bfloat16)
        await_bytes(tstat.at[t, pl.ds(0, devices - 1)], tssend.at[t])
        await_bytes(tpart.at[t, pl.ds(0, devices - 1)], tpsend.at[t])

    @pl.loop(shared - devices, shared)
    def _(i):
        settle(i)


def attend(axis, devices, q, k, v):
    n, tokens, heads, head = k.shape
    half = tokens * heads // 2
    k = k.reshape(n, 2, half, head)
    v = v.reshape(n, 2, half, head)
    tail = DIRECT
    shared = n - tail
    rounds = -(-shared // devices)
    dma = pltpu.SemaphoreType.DMA
    bf16, f32 = jnp.bfloat16, jnp.float32
    return pl.pallas_call(
        functools.partial(kernel, axis, devices, shared),
        out_shape=pltpu.VMEM((n, heads, head), bf16),
        in_specs=[pl.BlockSpec(memory_space=pl.ANY)] * 3,
        out_specs=pl.BlockSpec(memory_space=pltpu.VMEM),
        scratch_shapes=[
            pltpu.VMEM((n, heads, head), bf16),
            pltpu.VMEM((SLOTS, 2, half, head), bf16),
            pltpu.VMEM((SLOTS, 2, half, head), bf16),
            pltpu.VMEM((2, 2 * heads, half), f32),
            pltpu.VMEM((2, heads, LANES), f32),
            pltpu.VMEM((2, 2 * heads, half), bf16),
            pltpu.VMEM((shared, heads, head), bf16),
            pltpu.VMEM((shared, 2, LANES), f32),
            pltpu.VMEM((rounds, devices, heads, head), bf16),
            pltpu.VMEM((rounds, devices, 2, LANES), f32),
            pltpu.VMEM((tail, devices, heads, head), bf16),
            pltpu.VMEM((tail, devices, 2, LANES), f32),
            pltpu.VMEM((tail, devices, heads, head), f32),
            dma, dma((SLOTS,)), dma((SLOTS,)),
            dma((shared,)), dma((rounds,)), dma((shared,)), dma((rounds,)),
            dma((tail,)), dma((tail,)), dma((tail,)), dma((tail,)),
            dma((rounds,)), dma((shared,)),
        ],
        compiler_params=pltpu.CompilerParams(collective_id=0, has_side_effects=True, vmem_limit_bytes=56 << 20),
        name="attend",
    )(q, k, v)


def solution(mesh):
    def step(q, k, v):
        return attend("sp", mesh.shape["sp"], q, k, v)

    return jax.shard_map(
        step,
        mesh=mesh,
        in_specs=(P("dp", None, None), P("dp", "sp", None, None), P("dp", "sp", None, None)),
        out_specs=P("dp", None, None),
        check_vma=False,
    )
```
